128 devices in a mesh: head: 16 (over z_lo, y, core), row: 8 (over z_hi, x).
Axes of the slice: x: 4, y: 4, z: 4 (z_hi: 2, z_lo: 2; z = z_hi * 2 + z_lo), core: 2. Of those that a mesh axis runs over, the one named last changes fastest.
Arguments:
- token_ids: int32 [2048], replicated, may hold values from 0 to 151643, as said below
- teacher_hidden: bfloat16 [2048, 8192], P('head', 'row'), may hold values from -20 to 20
- teacher_query: bfloat16 [8192, 8192], P('row', 'head'), may hold values from -0.0625 to 0.0625
- teacher_kv: bfloat16 [8192, 2, 1024], P('row', None, 'head'), may hold values from -0.0625 to 0.0625
- student_hidden: bfloat16 [2048, 3584], P('head', 'row'), may hold values from -20 to 20
- student_query: bfloat16 [3584, 3584], P('row', 'head'), may hold values from -0.09375 to 0.09375
- student_kv: bfloat16 [3584, 2, 512], P('row', None, 'head'), may hold values from -0.09375 to 0.09375
Outputs:
- relation_loss: float32 [], replicated
- query_grad: float32 [3584, 3584], P('row', 'head')
- kv_grad: float32 [3584, 2, 512], P('row', None, 'head')
- hidden_grad: float32 [2048, 3584], P('head', 'row')
The draws below stay inside these ranges and needn't reach their ends.
Inputs may be any that keep to these rules, and one draw needn't show every extreme that they name: `token_ids`: from some position in the second half of the sequence on, if any, every position holds the padding id 151643; before it every id is below 151643.
All inputs are finite; a program needn't handle non-finite values.
Results may differ from the reference program's by a relative error of at most 0.0035.
The reference program's roundings to bfloat16 on the way (of `teacher_all`, `student_all`, `weights` and `vector_grad`) count: a program that leaves them out, or rounds other values in their place, can miss the bound.
Values may be sent and summed in bfloat16 or wider, within the bound.
A program may use at most 192 MiB of HBM per device.

```python
import jax
import jax.numpy as jnp
from jax import lax

DT = 8192
KVT = 1024
DS = 3584
KVS = 512
HEADS = 64
HDT = 128
KDT = 16
HDS = 56
KDS = 8
LEN = 2048


pad_token = 151643


def hidden_state(key, width, sigma):
    base_key = jax.random.fold_in(key, width)
    values = jax.random.truncated_normal(base_key, -4.0, 4.0, (LEN, width), jnp.float32) * sigma
    return values.astype(jnp.bfloat16)


def draw_token_ids(key, part):
    length = jax.random.randint(jax.random.fold_in(key, 5), (), LEN // 2, LEN + 1)
    words = jax.random.randint(jax.random.fold_in(key, 6), (LEN,), 0, pad_token)
    return jnp.where(jnp.arange(LEN) < length, words, pad_token).astype(jnp.int32)


def draw_teacher_hidden(key, part):
    return hidden_state(key, DT, 0.7)


def draw_student_hidden(key, part):
    return hidden_state(key, DS, 0.85)


def block_levels(key, dims, split, smallest, top_value):
    gain = 1.0
    for position, blocks in split:
        heights = jax.random.uniform(jax.random.fold_in(jax.random.fold_in(key, 6), position), (blocks,), jnp.float32, smallest / len(split), top_value / len(split))
        gain = gain * jnp.repeat(jnp.exp(heights), dims[position] // blocks).reshape((-1,) + (1,) * (len(dims) - 1 - position))
    return gain


def normal_values(key, extent, spread, limit, shards=(), dtype=jnp.bfloat16):
    values = jax.random.normal(key, extent, jnp.float32) * spread
    if len(shards) > 0:
        values = block_levels(key, extent, shards, -0.22, 0.18) * values
    return jnp.clip(values, min=-limit, max=limit).astype(dtype)


def setup_inputs(seed: int = 0) -> dict:
    splits = jax.random.split(jax.random.key(seed), 8)
    return {
        "token_ids": draw_token_ids(jax.random.fold_in(splits[7], 71), 0),
        "teacher_hidden": draw_teacher_hidden(jax.random.fold_in(splits[7], 71), 0),
        "teacher_query": normal_values(splits[2], (DT, DT), DT ** -0.5, 0.0625, ((0, 8), (1, 16))),
        "teacher_kv": normal_values(splits[3], (DT, 2, KVT), DT ** -0.5, 0.0625, ((0, 8), (2, 16))),
        "student_hidden": draw_student_hidden(jax.random.fold_in(splits[7], 71), 0),
        "student_query": normal_values(splits[5], (DS, DS), DS ** -0.5, 0.09375, ((0, 8), (1, 16))),
        "student_kv": normal_values(splits[6], (DS, 2, KVS), DS ** -0.5, 0.09375, ((0, 8), (2, 16))),
    }


pad_token = 151643
neg_fill = -1e30


def split_heads(matrix, first, head_dim):
    picked = matrix[:, first:first + HEADS * head_dim]
    return picked.reshape(picked.shape[0], HEADS, head_dim).transpose(1, 0, 2)


def reference(token_ids, teacher_hidden, teacher_query, teacher_kv, student_hidden, student_query, student_kv):
    valid_mask = token_ids != pad_token
    row_valid = valid_mask.astype(jnp.float32)
    teacher_weight = jnp.concatenate([teacher_query, teacher_kv.reshape(DT, 2 * KVT)], axis=1)
    student_weight = jnp.concatenate([student_query, student_kv.reshape(DS, 2 * KVS)], axis=1)
    teacher_all = jnp.dot(teacher_hidden, teacher_weight, preferred_element_type=jnp.float32).astype(jnp.bfloat16)
    student_all = jnp.dot(student_hidden, student_weight, preferred_element_type=jnp.float32).astype(jnp.bfloat16)
    kinds = [(0, HDT, 0, HDS), (DT, KDT, DS, KDS), (DT + KVT, KDT, DS + KVS, KDS)]

    loss_total = jnp.zeros((), jnp.float32)
    grad_kinds = []
    for teacher_first, teacher_dim, student_first, student_dim in kinds:
        teacher_scale = teacher_dim ** -0.5
        student_scale = student_dim ** -0.5

        def one_head(head_pair):
            teacher_vec, student_vec = head_pair
            teacher_logits = jnp.dot(teacher_vec, teacher_vec.T, preferred_element_type=jnp.float32) * teacher_scale
            teacher_logits = jnp.where(valid_mask[None, :], teacher_logits, neg_fill)
            teacher_log = jax.nn.log_softmax(teacher_logits, axis=-1)
            student_logits = jnp.dot(student_vec, student_vec.T, preferred_element_type=jnp.float32) * student_scale
            student_logits = jnp.where(valid_mask[None, :], student_logits, neg_fill)
            student_log = jax.nn.log_softmax(student_logits, axis=-1)
            teacher_prob = jnp.exp(teacher_log)
            student_prob = jnp.exp(student_log)
            loss_part = jnp.sum(jnp.sum(teacher_prob * (teacher_log - student_log), axis=1) * row_valid)
            weights = ((student_prob - teacher_prob) * row_valid[:, None]).astype(jnp.bfloat16)
            query_part = jnp.dot(weights, student_vec, preferred_element_type=jnp.float32) * student_scale
            key_part = jnp.dot(weights.T, student_vec, preferred_element_type=jnp.float32) * student_scale
            return loss_part, (query_part + key_part).astype(jnp.bfloat16)

        losses, grads = lax.map(one_head, (split_heads(teacher_all, teacher_first, teacher_dim), split_heads(student_all, student_first, student_dim)))
        loss_total = loss_total + jnp.sum(losses)
        grad_kinds.append(grads.transpose(1, 0, 2).reshape(LEN, HEADS * student_dim))
    vector_grad = jnp.concatenate(grad_kinds, axis=1)
    weight_grad = jnp.dot(student_hidden.T, vector_grad, preferred_element_type=jnp.float32)
    query_grad = weight_grad[:, :DS]
    kv_grad = weight_grad[:, DS:].reshape(DS, 2, KVS)
    hidden_grad = jnp.dot(vector_grad, student_weight.T, preferred_element_type=jnp.float32)
    relation_loss = loss_total / (3.0 * HEADS * jnp.sum(row_valid))
    return relation_loss, query_grad, kv_grad, hidden_grad
```

```python
import functools
import math

import jax
import jax.numpy as jnp
from jax import lax
from jax.experimental import pallas as pl
from jax.experimental.pallas import tpu as pltpu
from jax.sharding import Mesh
from jax.sharding import PartitionSpec as P

HEADS = 64
HEAD = ("head_0", "head_1", "head_2")
ROW = ("row_0", "row_1")

pad_token = 151643
neg_fill = -1e30
LOG2E = math.log2(math.e)
LN2 = math.log(2.0)

TILE = 256
GROUP = 32
LANES = 128


def relation_kernel(tdims, sdims, n_ref, p_ref, *refs):
    kinds = len(tdims)
    town, sown = refs[:kinds], refs[kinds : 2 * kinds]
    tall, sall = refs[2 * kinds : 3 * kinds], refs[3 * kinds : 4 * kinds]
    qp_ref, kp_ref, loss_ref, dt_ref, ds_ref, mt_ref, ms_ref, w_ref = refs[4 * kinds :]
    seq = tall[0].shape[1]
    step = pl.program_id(0)
    count = n_ref[0]
    first_row = (2 * step + p_ref[0]) * TILE

    @pl.when(step == 0)
    def _():
        kp_ref[...] = jnp.zeros_like(kp_ref)
        loss_ref[...] = jnp.zeros_like(loss_ref)

    @pl.when(first_row >= count)
    def _():
        qp_ref[...] = jnp.zeros_like(qp_ref)

    @pl.when(first_row < count)
    def _():
        at = 0
        for kind in range(kinds):
            scale_t = LOG2E * tdims[kind] ** (-0.5)
            scale_s = LOG2E * sdims[kind] ** (-0.5)
            for own, every, d_ref, m_ref in (
                (town[kind], tall[kind], dt_ref, mt_ref),
                (sown[kind], sall[kind], ds_ref, ms_ref),
            ):
                left = own[...]
                top = jnp.full((TILE, LANES), -jnp.inf, jnp.float32)
                for c in range(0, seq, TILE):
                    d = lax.dot_general(
                        left,
                        every[:, c : c + TILE],
                        (((0,), (0,)), ((), ())),
                        preferred_element_type=jnp.float32,
                    )
                    d_ref[:, c : c + TILE] = d
                    for k in range(0, TILE, LANES):
                        top = jnp.maximum(top, d[:, k : k + LANES])
                m_ref[...] = jnp.broadcast_to(
                    jnp.max(top, axis=1, keepdims=True), (TILE, LANES)
                )

            def group(g, loss):
                rows = pl.ds(pl.multiple_of(g * GROUP, GROUP), GROUP)
                mt, ms = mt_ref[rows, :], ms_ref[rows, :]
                zt = jnp.zeros((GROUP, LANES), jnp.float32)
                zs = jnp.zeros((GROUP, LANES), jnp.float32)
                kl = jnp.zeros((GROUP, LANES), jnp.float32)
                for c in range(0, seq, LANES):
                    xt = (dt_ref[rows, c : c + LANES] - mt) * scale_t
                    xs = (ds_ref[rows, c : c + LANES] - ms) * scale_s
                    et, es = jnp.exp2(xt), jnp.exp2(xs)
                    zt, zs, kl = zt + et, zs + es, kl + et * (xt - xs)
                    dt_ref[rows, c : c + LANES] = et
                    ds_ref[rows, c : c + LANES] = es
                zt = jnp.sum(zt, axis=1, keepdims=True)
                zs = jnp.sum(zs, axis=1, keepdims=True)
                kl = jnp.sum(kl, axis=1, keepdims=True)
                row = first_row + g * GROUP + lax.broadcasted_iota(jnp.int32, (GROUP, 1), 0)
                valid = row < count
                loss = loss + jnp.where(valid, kl / zt * LN2 + jnp.log(zs) - jnp.log(zt), 0.0)
                rt = jnp.broadcast_to(jnp.where(valid, 1.0 / zt, 0.0), (GROUP, LANES))
                rs = jnp.broadcast_to(jnp.where(valid, 1.0 / zs, 0.0), (GROUP, LANES))
                for c in range(0, seq, LANES):
                    w_ref[rows, c : c + LANES] = (
                        ds_ref[rows, c : c + LANES] * rs - dt_ref[rows, c : c + LANES] * rt
                    ).astype(jnp.bfloat16)
                return loss

            loss = lax.fori_loop(
                0, TILE // GROUP, group, jnp.zeros((GROUP, 1), jnp.float32)
            )
            loss_ref[...] += jnp.broadcast_to(loss, loss_ref.shape)
            width = sdims[kind]
            qp_ref[at : at + width, :] = lax.dot_general(
                sall[kind][...],
                w_ref[...],
                (((1,), (1,)), ((), ())),
                preferred_element_type=jnp.float32,
            )[:width]
            left = sown[kind][...]
            for c in range(0, seq, 2 * TILE):
                kp_ref[at : at + width, c : c + 2 * TILE] += lax.dot_general(
                    left,
                    w_ref[:, c : c + 2 * TILE],
                    (((1,), (0,)), ((), ())),
                    preferred_element_type=jnp.float32,
                )[:width]
            at += width


def relations(count, half, tdims, sdims, town, sown, tall, sall):
    seq = tall[0].shape[1]
    mine = town[0].shape[1]
    total = sum(sdims)
    block = lambda a: pl.BlockSpec((a.shape[0], TILE), lambda i: (0, i))
    whole = lambda a: pl.BlockSpec(a.shape, lambda i: (0, 0))
    smem = pl.BlockSpec(memory_space=pltpu.SMEM)
    return pl.pallas_call(
        functools.partial(relation_kernel, tdims, sdims),
        grid=(mine // TILE,),
        in_specs=[smem, smem]
        + [block(a) for a in town + sown]
        + [whole(a) for a in tall + sall],
        out_specs=[
            pl.BlockSpec((total, TILE), lambda i: (0, i)),
            pl.BlockSpec((total, seq), lambda i: (0, 0)),
            pl.BlockSpec((GROUP, LANES), lambda i: (0, 0)),
        ],
        out_shape=[
            jax.ShapeDtypeStruct((total, mine), jnp.float32),
            jax.ShapeDtypeStruct((total, seq), jnp.float32),
            jax.ShapeDtypeStruct((GROUP, LANES), jnp.float32),
        ],
        scratch_shapes=[
            pltpu.VMEM((TILE, seq), jnp.float32),
            pltpu.VMEM((TILE, seq), jnp.float32),
            pltpu.VMEM((TILE, LANES), jnp.float32),
            pltpu.VMEM((TILE, LANES), jnp.float32),
            pltpu.VMEM((TILE, seq), jnp.bfloat16),
        ],
        compiler_params=pltpu.CompilerParams(vmem_limit_bytes=40 * 2**20),
    )(count, half, *town, *sown, *tall, *sall)


def own_tokens(rows, half):
    cut = rows.reshape(rows.shape[0], -1, 2, TILE)
    return lax.dynamic_index_in_dim(cut, half, 2, keepdims=False).reshape(rows.shape[0], -1)


def by_head(query, kv, heads):
    feats = query.shape[0]
    parts = [
        query.reshape(feats, heads, -1),
        kv[:, 0].reshape(feats, heads, -1),
        kv[:, 1].reshape(feats, heads, -1),
    ]
    return jnp.concatenate(parts, axis=2)


def with_mask_row(rows, last):
    count = rows.shape[0]
    pad = -(count + 1) % 16
    return jnp.concatenate(
        [rows, last[None].astype(rows.dtype), jnp.zeros((pad, rows.shape[1]), rows.dtype)]
    )


def pieces(value):
    out = []
    for _ in range(3):
        top = lax.reduce_precision(value, 8, 7)
        out.append(top.astype(jnp.bfloat16))
        value = value - top
    return jnp.stack(out)


def copy_for_each(value, axis):
    size = lax.axis_size(axis)
    return lax.all_to_all(
        jnp.broadcast_to(value[None], (size, *value.shape)), axis, 0, 0, tiled=True
    )


def per_device(
    token_ids, teacher_hidden, teacher_query, teacher_kv, student_hidden, student_query, student_kv
):
    seq_len = token_ids.shape[0]
    local_heads = HEADS // lax.axis_size(HEAD)
    rows = lax.axis_size(ROW)
    me = lax.axis_index(ROW)
    half = me % 2
    valid_mask = token_ids != pad_token
    count = jnp.sum(valid_mask.astype(jnp.int32))

    both = jnp.concatenate([teacher_hidden, student_hidden], axis=1)
    feats = lax.all_gather(both, HEAD, axis=0, tiled=True)
    teacher_feats = feats[:, : teacher_hidden.shape[1]]
    student_feats = feats[:, teacher_hidden.shape[1] :]

    tdims = tuple(
        c // local_heads for c in (teacher_query.shape[1], teacher_kv.shape[2], teacher_kv.shape[2])
    )
    sdims = tuple(
        c // local_heads for c in (student_query.shape[1], student_kv.shape[2], student_kv.shape[2])
    )
    twidth, swidth = sum(tdims), sum(sdims)
    teacher_weight = by_head(teacher_query, teacher_kv, local_heads)
    student_weight = by_head(student_query, student_kv, local_heads)
    student_padded = jnp.pad(student_weight, ((0, 0), (0, 0), (0, -swidth % 16)))
    swidth_pad = student_padded.shape[2]
    project = lambda w, x: lax.dot_general(
        w.reshape(w.shape[0], -1),
        x,
        (((0,), (1,)), ((), ())),
        preferred_element_type=jnp.float32,
    )
    student_part = project(student_padded, student_feats)
    teacher_part = project(teacher_weight, teacher_feats)

    def reduced(part):
        arrived = lax.all_to_all(
            part.reshape(rows, -1, seq_len), ROW, split_axis=0, concat_axis=0, tiled=True
        )
        return arrived.sum(axis=0).astype(jnp.bfloat16)

    own_half = jnp.concatenate([reduced(teacher_part), reduced(student_part)])
    swap = [(i, i ^ 1) for i in range(lax.axis_size(ROW[1]))]
    other = lax.ppermute(own_half, ROW[1], swap)
    low = jnp.where(half == 0, own_half, other)
    high = jnp.where(half == 0, other, own_half)
    tcut = twidth // 2
    teacher_rows = jnp.concatenate([low[:tcut], high[:tcut]])
    student_rows = jnp.concatenate([low[tcut:], high[tcut:]])

    def cut(block, dims):
        out, at = [], 0
        for d in dims:
            out.append(block[at : at + d])
            at += d
        return out

    bias = jnp.where(valid_mask, 0.0, neg_fill)
    ones = jnp.ones((seq_len // 2,), jnp.float32)
    every = lambda parts: [with_mask_row(a, bias) for a in parts]
    mine = lambda parts: [with_mask_row(own_tokens(a, half), ones) for a in parts]
    tparts, sparts = cut(teacher_rows, tdims), cut(student_rows, sdims)
    query_part, key_part, loss = relations(
        count[None],
        half[None].astype(jnp.int32),
        tdims,
        sdims,
        mine(tparts),
        mine(sparts),
        every(tparts),
        every(sparts),
    )
    loss_sum = jnp.sum(loss[:, 0])
    from_other = lax.ppermute(own_tokens(key_part, 1 - half), ROW[1], swap)
    scale = jnp.concatenate([jnp.full((d, 1), d ** (-0.5), jnp.float32) for d in sdims])
    grad_own = ((query_part + own_tokens(key_part, half) + from_other) * scale).astype(jnp.bfloat16)
    below = -swidth % 16
    extra = jnp.zeros((below, grad_own.shape[1]), jnp.bfloat16).at[0, :3].set(pieces(loss_sum))
    arrived = copy_for_each(jnp.concatenate([grad_own, extra]), ROW)
    row_loss = jnp.sum(arrived[:, swidth, :3].astype(jnp.float32))
    grads = (
        arrived[:, :swidth].reshape(local_heads, 2, swidth, -1, TILE)
        .transpose(0, 2, 3, 1, 4)
        .reshape(local_heads * swidth, seq_len)
    )
    weight_grad = lax.dot_general(
        student_feats, grads, (((0,), (1,)), ((), ())), preferred_element_type=jnp.float32
    ).reshape(student_feats.shape[1], local_heads, swidth)
    q, k = sdims[0], sdims[1]
    query_out = weight_grad[:, :, :q].reshape(student_query.shape)
    kv_out = jnp.stack(
        [
            weight_grad[:, :, q : q + k].reshape(-1, local_heads * k),
            weight_grad[:, :, q + k :].reshape(-1, local_heads * k),
        ],
        axis=1,
    )

    heads = lax.axis_size(HEAD)
    all_weight = lax.all_gather(
        student_weight.reshape(student_weight.shape[0], -1).T, HEAD, axis=0, tiled=True
    )
    blocks = jnp.moveaxis(grads.reshape(grads.shape[0], heads, -1), 1, 0)
    extra = jnp.zeros((16, blocks.shape[2]), jnp.bfloat16).at[0, :3].set(pieces(row_loss))
    sent = jnp.concatenate([blocks, jnp.broadcast_to(extra[None], (heads, *extra.shape))], axis=1)
    got = lax.all_to_all(sent, HEAD, split_axis=0, concat_axis=0, tiled=True)
    kl_sum = jnp.sum(got[:, grads.shape[0], :3].astype(jnp.float32))
    input_grad = lax.dot_general(
        got[:, : grads.shape[0]].reshape(heads * grads.shape[0], -1),
        all_weight,
        (((0,), (0,)), ((), ())),
        preferred_element_type=jnp.float32,
    )
    mean_kl = kl_sum / (3.0 * HEADS * count.astype(jnp.float32))
    return (mean_kl, query_out, kv_out, input_grad)


def solution(mesh):
    finer = Mesh(
        mesh.devices.reshape(2, 4, 2, 2, 4), ("head_0", "head_1", "head_2", "row_0", "row_1")
    )
    in_specs = (
        P(),
        P(HEAD, ROW),
        P(ROW, HEAD),
        P(ROW, None, HEAD),
        P(HEAD, ROW),
        P(ROW, HEAD),
        P(ROW, None, HEAD),
    )
    out_specs = (P(), P(ROW, HEAD), P(ROW, None, HEAD), P(HEAD, ROW))
    return jax.shard_map(
        per_device, mesh=finer, in_specs=in_specs, out_specs=out_specs, check_vma=False
    )
```

```python
import functools
import math

import jax
import jax.numpy as jnp
from jax import lax
from jax.experimental import pallas as pl
from jax.experimental.pallas import tpu as pltpu
from jax.sharding import Mesh
from jax.sharding import PartitionSpec as P

HEADS = 64
HEAD = ("head_0", "head_1", "head_2")
ROW = ("row_0", "row_1")

pad_token = 151643
neg_fill = -1e30
LOG2E = math.log2(math.e)
LN2 = math.log(2.0)

TILE = 256
GROUP = 32
LANES = 128


def relation_kernel(tdims, sdims, n_ref, p_ref, *refs):
    kinds = len(tdims)
    town, sown = refs[:kinds], refs[kinds : 2 * kinds]
    tall, sall = refs[2 * kinds : 3 * kinds], refs[3 * kinds : 4 * kinds]
    qp_ref, kp_ref, loss_ref, dt_ref, ds_ref, mt_ref, ms_ref, w_ref = refs[4 * kinds :]
    seq = tall[0].shape[1]
    step = pl.program_id(0)
    count = n_ref[0]
    first_row = (2 * step + p_ref[0]) * TILE

    @pl.when(step == 0)
    def _():
        kp_ref[...] = jnp.zeros_like(kp_ref)
        loss_ref[...] = jnp.zeros_like(loss_ref)

    @pl.when(first_row >= count)
    def _():
        qp_ref[...] = jnp.zeros_like(qp_ref)

    @pl.when(first_row < count)
    def _():
        at = 0
        for kind in range(kinds):
            scale_t = LOG2E * tdims[kind] ** (-0.5)
            scale_s = LOG2E * sdims[kind] ** (-0.5)
            for own, every, d_ref, m_ref in (
                (town[kind], tall[kind], dt_ref, mt_ref),
                (sown[kind], sall[kind], ds_ref, ms_ref),
            ):
                left = own[...]
                top = jnp.full((TILE, LANES), -jnp.inf, jnp.float32)
                for c in range(0, seq, TILE):
                    d = lax.dot_general(
                        left,
                        every[:, c : c + TILE],
                        (((0,), (0,)), ((), ())),
                        preferred_element_type=jnp.float32,
                    )
                    d_ref[:, c : c + TILE] = d
                    for k in range(0, TILE, LANES):
                        top = jnp.maximum(top, d[:, k : k + LANES])
                m_ref[...] = jnp.broadcast_to(
                    jnp.max(top, axis=1, keepdims=True), (TILE, LANES)
                )

            def group(g, loss):
                rows = pl.ds(pl.multiple_of(g * GROUP, GROUP), GROUP)
                mt, ms = mt_ref[rows, :], ms_ref[rows, :]
                zt = jnp.zeros((GROUP, LANES), jnp.float32)
                zs = jnp.zeros((GROUP, LANES), jnp.float32)
                kl = jnp.zeros((GROUP, LANES), jnp.float32)
                for c in range(0, seq, LANES):
                    xt = (dt_ref[rows, c : c + LANES] - mt) * scale_t
                    xs = (ds_ref[rows, c : c + LANES] - ms) * scale_s
                    et, es = jnp.exp2(xt), jnp.exp2(xs)
                    zt, zs, kl = zt + et, zs + es, kl + et * (xt - xs)
                    dt_ref[rows, c : c + LANES] = et
                    ds_ref[rows, c : c + LANES] = es
                zt = jnp.sum(zt, axis=1, keepdims=True)
                zs = jnp.sum(zs, axis=1, keepdims=True)
                kl = jnp.sum(kl, axis=1, keepdims=True)
                row = first_row + g * GROUP + lax.broadcasted_iota(jnp.int32, (GROUP, 1), 0)
                valid = row < count
                loss = loss + jnp.where(valid, kl / zt * LN2 + jnp.log(zs) - jnp.log(zt), 0.0)
                rt = jnp.broadcast_to(jnp.where(valid, 1.0 / zt, 0.0), (GROUP, LANES))
                rs = jnp.broadcast_to(jnp.where(valid, 1.0 / zs, 0.0), (GROUP, LANES))
                for c in range(0, seq, LANES):
                    w_ref[rows, c : c + LANES] = (
                        ds_ref[rows, c : c + LANES] * rs - dt_ref[rows, c : c + LANES] * rt
                    ).astype(jnp.bfloat16)
                return loss

            loss = lax.fori_loop(
                0, TILE // GROUP, group, jnp.zeros((GROUP, 1), jnp.float32)
            )
            loss_ref[...] += jnp.broadcast_to(loss, loss_ref.shape)
            width = sdims[kind]
            qp_ref[at : at + width, :] = lax.dot_general(
                sall[kind][...],
                w_ref[...],
                (((1,), (1,)), ((), ())),
                preferred_element_type=jnp.float32,
            )[:width]
            left = sown[kind][...]
            for c in range(0, seq, 2 * TILE):
                kp_ref[at : at + width, c : c + 2 * TILE] += lax.dot_general(
                    left,
                    w_ref[:, c : c + 2 * TILE],
                    (((1,), (0,)), ((), ())),
                    preferred_element_type=jnp.float32,
                )[:width]
            at += width


def relations(count, half, tdims, sdims, town, sown, tall, sall):
    seq = tall[0].shape[1]
    mine = town[0].shape[1]
    total = sum(sdims)
    block = lambda a: pl.BlockSpec((a.shape[0], TILE), lambda i: (0, i))
    whole = lambda a: pl.BlockSpec(a.shape, lambda i: (0, 0))
    smem = pl.BlockSpec(memory_space=pltpu.SMEM)
    return pl.pallas_call(
        functools.partial(relation_kernel, tdims, sdims),
        grid=(mine // TILE,),
        in_specs=[smem, smem]
        + [block(a) for a in town + sown]
        + [whole(a) for a in tall + sall],
        out_specs=[
            pl.BlockSpec((total, TILE), lambda i: (0, i)),
            pl.BlockSpec((total, seq), lambda i: (0, 0)),
            pl.BlockSpec((GROUP, LANES), lambda i: (0, 0)),
        ],
        out_shape=[
            jax.ShapeDtypeStruct((total, mine), jnp.float32),
            jax.ShapeDtypeStruct((total, seq), jnp.float32),
            jax.ShapeDtypeStruct((GROUP, LANES), jnp.float32),
        ],
        scratch_shapes=[
            pltpu.VMEM((TILE, seq), jnp.float32),
            pltpu.VMEM((TILE, seq), jnp.float32),
            pltpu.VMEM((TILE, LANES), jnp.float32),
            pltpu.VMEM((TILE, LANES), jnp.float32),
            pltpu.VMEM((TILE, seq), jnp.bfloat16),
        ],
        compiler_params=pltpu.CompilerParams(vmem_limit_bytes=40 * 2**20),
        cost_estimate=pl.CostEstimate(
            flops=len(tdims) * 10_000_000_000, bytes_accessed=4 * 2**20, transcendentals=0
        ),
    )(count, half, *town, *sown, *tall, *sall)


def own_tokens(rows, half):
    cut = rows.reshape(rows.shape[0], -1, 2, TILE)
    return lax.dynamic_index_in_dim(cut, half, 2, keepdims=False).reshape(rows.shape[0], -1)


def columns_of_heads(parts, heads, pad):
    feats = parts[0].shape[0]
    joined = jnp.concatenate([a.reshape(feats, heads, -1) for a in parts], axis=2)
    joined = jnp.pad(joined, ((0, 0), (0, 0), (0, pad - joined.shape[2])))
    return joined.reshape(feats, -1)


def with_mask_row(rows, last):
    count = rows.shape[0]
    pad = -(count + 1) % 16
    return jnp.concatenate(
        [rows, last[None].astype(rows.dtype), jnp.zeros((pad, rows.shape[1]), rows.dtype)]
    )


def pieces(value):
    out = []
    for _ in range(3):
        top = lax.reduce_precision(value, 8, 7)
        out.append(top.astype(jnp.bfloat16))
        value = value - top
    return jnp.stack(out)


def copy_for_each(value, axis):
    size = lax.axis_size(axis)
    return lax.all_to_all(
        jnp.broadcast_to(value[None], (size, *value.shape)), axis, 0, 0, tiled=True
    )


def per_device(
    token_ids, teacher_hidden, teacher_query, teacher_kv, student_hidden, student_query, student_kv
):
    seq_len = token_ids.shape[0]
    heads = lax.axis_size(HEAD)
    local_heads = HEADS // heads
    rows = lax.axis_size(ROW)
    half = lax.axis_index(ROW) % 2
    swap = [(i, i ^ 1) for i in range(lax.axis_size(ROW[1]))]
    valid_mask = token_ids != pad_token
    count = jnp.sum(valid_mask.astype(jnp.int32))
    bias = jnp.where(valid_mask, 0.0, neg_fill)
    ones = jnp.ones((seq_len // 2,), jnp.float32)

    tq, tk = teacher_query.shape[1] // local_heads, teacher_kv.shape[2] // local_heads
    sq, sk = student_query.shape[1] // local_heads, student_kv.shape[2] // local_heads
    q_pad = sq + -sq % 16
    s_pad = q_pad + 2 * sk
    student_parts = [student_query, student_kv[:, 0], student_kv[:, 1]]
    student_weight = columns_of_heads(student_parts, local_heads, s_pad)
    teacher_kv_weight = columns_of_heads([teacher_kv[:, 0], teacher_kv[:, 1]], local_heads, 2 * tk)

    def project(weight, feats):
        return lax.dot_general(
            weight, feats, (((0,), (1,)), ((), ())), preferred_element_type=jnp.float32
        )

    def swapped(own):
        other = lax.ppermute(own, ROW[1], swap)
        low = jnp.where(half == 0, own, other)
        high = jnp.where(half == 0, other, own)
        return jnp.concatenate([low, high])

    def reduced(part):
        arrived = lax.all_to_all(
            part.reshape(rows, -1, seq_len), ROW, split_axis=0, concat_axis=0, tiled=True
        )
        return swapped(arrived.sum(axis=0).astype(jnp.bfloat16))

    student_feats = lax.all_gather(student_hidden, HEAD, axis=0, tiled=True)
    teacher_feats = lax.all_gather(teacher_hidden, HEAD, axis=0, tiled=True)
    student_rows = reduced(project(student_weight, student_feats))
    teacher_kv_rows = reduced(project(teacher_kv_weight, teacher_feats))
    teacher_q_rows = reduced(project(teacher_query, teacher_feats))

    def relate(tparts, sparts):
        every = lambda parts: [with_mask_row(a, bias) for a in parts]
        mine = lambda parts: [with_mask_row(own_tokens(a, half), ones) for a in parts]
        tdims, sdims = tuple(a.shape[0] for a in tparts), tuple(a.shape[0] for a in sparts)
        query_part, key_part, loss = relations(
            count[None],
            half[None].astype(jnp.int32),
            tdims,
            sdims,
            mine(tparts),
            mine(sparts),
            every(tparts),
            every(sparts),
        )
        from_other = lax.ppermute(own_tokens(key_part, 1 - half), ROW[1], swap)
        scale = jnp.concatenate([jnp.full((d, 1), d ** (-0.5), jnp.float32) for d in sdims])
        grad = (query_part + own_tokens(key_part, half) + from_other) * scale
        return grad.astype(jnp.bfloat16), jnp.sum(loss[:, 0])

    def shared(grad):
        arrived = copy_for_each(grad, ROW)
        cut = arrived.reshape(local_heads, 2, grad.shape[0], -1, TILE // LANES, LANES)
        return cut.transpose(3, 1, 4, 0, 2, 5).reshape(heads, -1, LANES)

    def weight_grads(blocks):
        by_column = jnp.moveaxis(blocks, 0, 1).reshape(blocks.shape[1], seq_len)
        return lax.dot_general(
            student_feats, by_column, (((0,), (1,)), ((), ())), preferred_element_type=jnp.float32
        ).reshape(student_feats.shape[1], local_heads, -1)

    def token_grads(blocks, weight):
        got = lax.all_to_all(blocks, HEAD, split_axis=0, concat_axis=0, tiled=True)
        flat = got.reshape(-1, got.shape[2])
        return got, lax.dot_general(
            flat,
            weight.reshape(flat.shape[0], -1),
            (((0,), (0,)), ((), ())),
            preferred_element_type=jnp.float32,
        )

    spread = jnp.concatenate(
        [
            columns_of_heads(student_parts[:1], local_heads, q_pad).T,
            columns_of_heads(student_parts[1:], local_heads, 2 * sk).T,
        ]
    )
    all_weight = lax.all_gather(spread, HEAD, axis=0, tiled=False)

    kv_grad, kv_loss = relate(
        [teacher_kv_rows[:tk], teacher_kv_rows[tk:]],
        [student_rows[sq : sq + sk], student_rows[sq + sk : sq + 2 * sk]],
    )
    kv_blocks = shared(kv_grad)
    kv_out = (
        weight_grads(kv_blocks)
        .reshape(-1, local_heads, 2, sk)
        .transpose(0, 2, 1, 3)
        .reshape(student_kv.shape)
    )
    _, kv_input = token_grads(kv_blocks, all_weight[:, local_heads * q_pad :])

    q_grad, q_loss = relate([teacher_q_rows], [student_rows[:sq]])
    loss = q_loss + kv_loss
    loss = pieces(loss + lax.ppermute(loss, ROW[1], swap))
    last = jnp.zeros((q_pad - sq, q_grad.shape[1] // LANES, LANES), jnp.bfloat16)
    last = last.at[0, :, :3].set(jnp.broadcast_to(loss, (last.shape[1], 3)))
    q_blocks = shared(jnp.concatenate([q_grad, last.reshape(q_pad - sq, -1)]))
    query_out = weight_grads(q_blocks)[:, :, :sq].reshape(student_query.shape)
    got, q_input = token_grads(q_blocks, all_weight[:, : local_heads * q_pad])
    kl_sum = jnp.sum(got.reshape(heads, local_heads, q_pad, LANES)[:, :, sq, :3].astype(jnp.float32))
    mean_kl = kl_sum / (3.0 * HEADS * count.astype(jnp.float32))
    return (mean_kl, query_out, kv_out, kv_input + q_input)


def solution(mesh):
    finer = Mesh(
        mesh.devices.reshape(2, 4, 2, 2, 4), ("head_0", "head_1", "head_2", "row_0", "row_1")
    )
    in_specs = (
        P(),
        P(HEAD, ROW),
        P(ROW, HEAD),
        P(ROW, None, HEAD),
        P(HEAD, ROW),
        P(ROW, HEAD),
        P(ROW, None, HEAD),
    )
    out_specs = (P(), P(ROW, HEAD), P(ROW, None, HEAD), P(HEAD, ROW))
    return jax.shard_map(
        per_device, mesh=finer, in_specs=in_specs, out_specs=out_specs, check_vma=False
    )
```

```python
import functools
import math

import jax
import jax.numpy as jnp
from jax import lax
from jax.experimental import pallas as pl
from jax.experimental.pallas import tpu as pltpu
from jax.sharding import Mesh
from jax.sharding import PartitionSpec as P

HEADS = 64
HEAD = ("head_0", "head_1", "head_2")
ROW = ("row_0", "row_1")

pad_token = 151643
neg_fill = -1e30
LOG2E = math.log2(math.e)
LN2 = math.log(2.0)

TILE = 256
GROUP = 32
LANES = 128


def relation_kernel(tdims, sdims, n_ref, p_ref, *refs):
    kinds = len(tdims)
    town, sown = refs[:kinds], refs[kinds : 2 * kinds]
    tall, sall = refs[2 * kinds : 3 * kinds], refs[3 * kinds : 4 * kinds]
    qp_ref, kp_ref, loss_ref, dt_ref, ds_ref, mt_ref, ms_ref, w_ref = refs[4 * kinds :]
    seq = tall[0].shape[1]
    step = pl.program_id(0)
    count = n_ref[0]
    first_row = (2 * step + p_ref[0]) * TILE

    @pl.when(step == 0)
    def _():
        kp_ref[...] = jnp.zeros_like(kp_ref)
        loss_ref[...] = jnp.zeros_like(loss_ref)

    @pl.when(first_row >= count)
    def _():
        qp_ref[...] = jnp.zeros_like(qp_ref)

    @pl.when(first_row < count)
    def _():
        at = 0
        for kind in range(kinds):
            scale_t = LOG2E * tdims[kind] ** (-0.5)
            scale_s = LOG2E * sdims[kind] ** (-0.5)
            for own, every, d_ref, m_ref in (
                (town[kind], tall[kind], dt_ref, mt_ref),
                (sown[kind], sall[kind], ds_ref, ms_ref),
            ):
                left = own[...]
                top = jnp.full((TILE, LANES), -jnp.inf, jnp.float32)
                for c in range(0, seq, TILE):
                    d = lax.dot_general(
                        left,
                        every[:, c : c + TILE],
                        (((0,), (0,)), ((), ())),
                        preferred_element_type=jnp.float32,
                    )
                    d_ref[:, c : c + TILE] = d
                    for k in range(0, TILE, LANES):
                        top = jnp.maximum(top, d[:, k : k + LANES])
                m_ref[...] = jnp.broadcast_to(
                    jnp.max(top, axis=1, keepdims=True), (TILE, LANES)
                )

            def group(g, loss):
                rows = pl.ds(pl.multiple_of(g * GROUP, GROUP), GROUP)
                mt, ms = mt_ref[rows, :], ms_ref[rows, :]
                zt = jnp.zeros((GROUP, LANES), jnp.float32)
                zs = jnp.zeros((GROUP, LANES), jnp.float32)
                kl = jnp.zeros((GROUP, LANES), jnp.float32)
                for c in range(0, seq, LANES):
                    xt = (dt_ref[rows, c : c + LANES] - mt) * scale_t
                    xs = (ds_ref[rows, c : c + LANES] - ms) * scale_s
                    et, es = jnp.exp2(xt), jnp.exp2(xs)
                    zt, zs, kl = zt + et, zs + es, kl + et * (xt - xs)
                    dt_ref[rows, c : c + LANES] = et
                    ds_ref[rows, c : c + LANES] = es
                zt = jnp.sum(zt, axis=1, keepdims=True)
                zs = jnp.sum(zs, axis=1, keepdims=True)
                kl = jnp.sum(kl, axis=1, keepdims=True)
                row = first_row + g * GROUP + lax.broadcasted_iota(jnp.int32, (GROUP, 1), 0)
                valid = row < count
                loss = loss + jnp.where(valid, kl / zt * LN2 + jnp.log(zs) - jnp.log(zt), 0.0)
                rt = jnp.broadcast_to(jnp.where(valid, 1.0 / zt, 0.0), (GROUP, LANES))
                rs = jnp.broadcast_to(jnp.where(valid, 1.0 / zs, 0.0), (GROUP, LANES))
                for c in range(0, seq, LANES):
                    w_ref[rows, c : c + LANES] = (
                        ds_ref[rows, c : c + LANES] * rs - dt_ref[rows, c : c + LANES] * rt
                    ).astype(jnp.bfloat16)
                return loss

            loss = lax.fori_loop(
                0, TILE // GROUP, group, jnp.zeros((GROUP, 1), jnp.float32)
            )
            loss_ref[...] += jnp.broadcast_to(loss, loss_ref.shape)
            width = sdims[kind]
            qp_ref[at : at + width, :] = lax.dot_general(
                sall[kind][...],
                w_ref[...],
                (((1,), (1,)), ((), ())),
                preferred_element_type=jnp.float32,
            )[:width]
            left = sown[kind][...]
            for c in range(0, seq, 2 * TILE):
                kp_ref[at : at + width, c : c + 2 * TILE] += lax.dot_general(
                    left,
                    w_ref[:, c : c + 2 * TILE],
                    (((1,), (0,)), ((), ())),
                    preferred_element_type=jnp.float32,
                )[:width]
            at += width


def relations(count, half, tdims, sdims, town, sown, tall, sall):
    seq = tall[0].shape[1]
    mine = town[0].shape[1]
    total = sum(sdims)
    block = lambda a: pl.BlockSpec((a.shape[0], TILE), lambda i: (0, i))
    whole = lambda a: pl.BlockSpec(a.shape, lambda i: (0, 0))
    smem = pl.BlockSpec(memory_space=pltpu.SMEM)
    return pl.pallas_call(
        functools.partial(relation_kernel, tdims, sdims),
        grid=(mine // TILE,),
        in_specs=[smem, smem]
        + [block(a) for a in town + sown]
        + [whole(a) for a in tall + sall],
        out_specs=[
            pl.BlockSpec((total, TILE), lambda i: (0, i)),
            pl.BlockSpec((total, seq), lambda i: (0, 0)),
            pl.BlockSpec((GROUP, LANES), lambda i: (0, 0)),
        ],
        out_shape=[
            jax.ShapeDtypeStruct((total, mine), jnp.float32),
            jax.ShapeDtypeStruct((total, seq), jnp.float32),
            jax.ShapeDtypeStruct((GROUP, LANES), jnp.float32),
        ],
        scratch_shapes=[
            pltpu.VMEM((TILE, seq), jnp.float32),
            pltpu.VMEM((TILE, seq), jnp.float32),
            pltpu.VMEM((TILE, LANES), jnp.float32),
            pltpu.VMEM((TILE, LANES), jnp.float32),
            pltpu.VMEM((TILE, seq), jnp.bfloat16),
        ],
        compiler_params=pltpu.CompilerParams(vmem_limit_bytes=40 * 2**20),
        cost_estimate=pl.CostEstimate(
            flops=len(tdims) * 10_000_000_000, bytes_accessed=4 * 2**20, transcendentals=0
        ),
    )(count, half, *town, *sown, *tall, *sall)


def own_tokens(rows, half):
    cut = rows.reshape(rows.shape[0], -1, 2, TILE)
    return lax.dynamic_index_in_dim(cut, half, 2, keepdims=False).reshape(rows.shape[0], -1)


def columns_of_heads(parts, heads, pad):
    feats = parts[0].shape[0]
    joined = jnp.concatenate([a.reshape(feats, heads, -1) for a in parts], axis=2)
    joined = jnp.pad(joined, ((0, 0), (0, 0), (0, pad - joined.shape[2])))
    return joined.reshape(feats, -1)


def with_mask_row(rows, last):
    count = rows.shape[0]
    pad = -(count + 1) % 16
    return jnp.concatenate(
        [rows, last[None].astype(rows.dtype), jnp.zeros((pad, rows.shape[1]), rows.dtype)]
    )


def pieces(value):
    out = []
    for _ in range(3):
        top = lax.reduce_precision(value, 8, 7)
        out.append(top.astype(jnp.bfloat16))
        value = value - top
    return jnp.stack(out)


def copy_for_each(value, axis):
    size = lax.axis_size(axis)
    return lax.all_to_all(
        jnp.broadcast_to(value[None], (size, *value.shape)), axis, 0, 0, tiled=True
    )


def per_device(
    token_ids, teacher_hidden, teacher_query, teacher_kv, student_hidden, student_query, student_kv
):
    seq_len = token_ids.shape[0]
    heads = lax.axis_size(HEAD)
    local_heads = HEADS // heads
    rows = lax.axis_size(ROW)
    half = lax.axis_index(ROW) % 2
    swap = [(i, i ^ 1) for i in range(lax.axis_size(ROW[1]))]
    valid_mask = token_ids != pad_token
    count = jnp.sum(valid_mask.astype(jnp.int32))
    bias = jnp.where(valid_mask, 0.0, neg_fill)
    ones = jnp.ones((seq_len // 2,), jnp.float32)

    tq, tk = teacher_query.shape[1] // local_heads, teacher_kv.shape[2] // local_heads
    sq, sk = student_query.shape[1] // local_heads, student_kv.shape[2] // local_heads
    q_pad = sq + -sq % 16
    s_pad = q_pad + 2 * sk
    student_parts = [student_query, student_kv[:, 0], student_kv[:, 1]]
    student_weight = columns_of_heads(student_parts, local_heads, s_pad)
    teacher_kv_weight = columns_of_heads([teacher_kv[:, 0], teacher_kv[:, 1]], local_heads, 2 * tk)

    def project(weight, feats):
        return lax.dot_general(
            weight, feats, (((0,), (1,)), ((), ())), preferred_element_type=jnp.float32
        )

    def swapped(own):
        other = lax.ppermute(own, ROW[1], swap)
        low = jnp.where(half == 0, own, other)
        high = jnp.where(half == 0, other, own)
        return jnp.concatenate([low, high])

    def reduced(part):
        arrived = lax.all_to_all(part, ROW, split_axis=0, concat_axis=0, tiled=True)
        return arrived.sum(axis=0).astype(jnp.bfloat16)

    for_rows = lambda part: part.reshape(rows, -1, seq_len)
    both = jnp.concatenate([teacher_hidden, student_hidden], axis=1)
    feats = lax.all_gather(both, HEAD, axis=0, tiled=True)
    teacher_feats = feats[:, : teacher_hidden.shape[1]]
    student_feats = feats[:, teacher_hidden.shape[1] :]
    first = jnp.concatenate(
        [
            for_rows(project(student_weight, student_feats)),
            for_rows(project(teacher_kv_weight, teacher_feats)),
        ],
        axis=1,
    )
    first_rows = swapped(reduced(first))
    cut = first_rows.reshape(2, -1, seq_len)
    student_rows = cut[:, : local_heads * s_pad // rows].reshape(-1, seq_len)
    teacher_kv_rows = cut[:, local_heads * s_pad // rows :].reshape(-1, seq_len)
    second = for_rows(project(teacher_query, teacher_feats))
    second, student_rows, teacher_kv_rows = lax.optimization_barrier(
        (second, student_rows, teacher_kv_rows)
    )
    teacher_q_rows = swapped(reduced(second))

    def relate(tparts, sparts):
        every = lambda parts: [with_mask_row(a, bias) for a in parts]
        mine = lambda parts: [with_mask_row(own_tokens(a, half), ones) for a in parts]
        tdims, sdims = tuple(a.shape[0] for a in tparts), tuple(a.shape[0] for a in sparts)
        query_part, key_part, loss = relations(
            count[None],
            half[None].astype(jnp.int32),
            tdims,
            sdims,
            mine(tparts),
            mine(sparts),
            every(tparts),
            every(sparts),
        )
        from_other = lax.ppermute(own_tokens(key_part, 1 - half), ROW[1], swap)
        scale = jnp.concatenate([jnp.full((d, 1), d ** (-0.5), jnp.float32) for d in sdims])
        grad = (query_part + own_tokens(key_part, half) + from_other) * scale
        return grad.astype(jnp.bfloat16), jnp.sum(loss[:, 0])

    def shared(grad):
        arrived = copy_for_each(grad, ROW)
        cut = arrived.reshape(local_heads, 2, grad.shape[0], -1, TILE // LANES, LANES)
        return cut.transpose(3, 1, 4, 0, 2, 5).reshape(heads, -1, LANES)

    def weight_grads(blocks):
        by_column = jnp.moveaxis(blocks, 0, 1).reshape(blocks.shape[1], seq_len)
        return lax.dot_general(
            student_feats, by_column, (((0,), (1,)), ((), ())), preferred_element_type=jnp.float32
        ).reshape(student_feats.shape[1], local_heads, -1)

    def token_grads(blocks, weight):
        got = lax.all_to_all(blocks, HEAD, split_axis=0, concat_axis=0, tiled=True)
        flat = got.reshape(-1, got.shape[2])
        return got, lax.dot_general(
            flat,
            weight.reshape(flat.shape[0], -1),
            (((0,), (0,)), ((), ())),
            preferred_element_type=jnp.float32,
        )

    spread = jnp.concatenate(
        [
            columns_of_heads(student_parts[:1], local_heads, q_pad).T,
            columns_of_heads(student_parts[1:], local_heads, 2 * sk).T,
        ]
    )
    all_weight = lax.all_gather(spread, HEAD, axis=0, tiled=False)

    kv_grad, kv_loss = relate(
        [teacher_kv_rows[:tk], teacher_kv_rows[tk:]],
        [student_rows[sq : sq + sk], student_rows[sq + sk : sq + 2 * sk]],
    )
    kv_blocks = shared(kv_grad)
    kv_out = (
        weight_grads(kv_blocks)
        .reshape(-1, local_heads, 2, sk)
        .transpose(0, 2, 1, 3)
        .reshape(student_kv.shape)
    )
    _, kv_input = token_grads(kv_blocks, all_weight[:, local_heads * q_pad :])

    q_grad, q_loss = relate([teacher_q_rows], [student_rows[:sq]])
    loss = q_loss + kv_loss
    loss = pieces(loss + lax.ppermute(loss, ROW[1], swap))
    last = jnp.zeros((q_pad - sq, q_grad.shape[1] // LANES, LANES), jnp.bfloat16)
    last = last.at[0, :, :3].set(jnp.broadcast_to(loss, (last.shape[1], 3)))
    q_blocks = shared(jnp.concatenate([q_grad, last.reshape(q_pad - sq, -1)]))
    query_out = weight_grads(q_blocks)[:, :, :sq].reshape(student_query.shape)
    got, q_input = token_grads(q_blocks, all_weight[:, : local_heads * q_pad])
    kl_sum = jnp.sum(got.reshape(heads, local_heads, q_pad, LANES)[:, :, sq, :3].astype(jnp.float32))
    mean_kl = kl_sum / (3.0 * HEADS * count.astype(jnp.float32))
    return (mean_kl, query_out, kv_out, kv_input + q_input)


def solution(mesh):
    finer = Mesh(
        mesh.devices.reshape(2, 4, 2, 2, 4), ("head_0", "head_1", "head_2", "row_0", "row_1")
    )
    in_specs = (
        P(),
        P(HEAD, ROW),
        P(ROW, HEAD),
        P(ROW, None, HEAD),
        P(HEAD, ROW),
        P(ROW, HEAD),
        P(ROW, None, HEAD),
    )
    out_specs = (P(), P(ROW, HEAD), P(ROW, None, HEAD), P(HEAD, ROW))
    return jax.shard_map(
        per_device, mesh=finer, in_specs=in_specs, out_specs=out_specs, check_vma=False
    )
```

```python
import functools
import math

import jax
import jax.numpy as jnp
from jax import lax
from jax.experimental import pallas as pl
from jax.experimental.pallas import tpu as pltpu
from jax.sharding import Mesh
from jax.sharding import PartitionSpec as P

HEADS = 64
HEAD = ("head_0", "head_1", "head_2")
ROW = ("row_0", "row_1")

pad_token = 151643
neg_fill = -1e30
LOG2E = math.log2(math.e)
LN2 = math.log(2.0)

TILE = 256
GROUP = 32
LANES = 128


def relation_kernel(tdims, sdims, n_ref, p_ref, *refs):
    kinds = len(tdims)
    town, sown = refs[:kinds], refs[kinds : 2 * kinds]
    tall, sall = refs[2 * kinds : 3 * kinds], refs[3 * kinds : 4 * kinds]
    qp_ref, kp_ref, loss_ref, dt_ref, ds_ref, mt_ref, ms_ref, w_ref = refs[4 * kinds :]
    seq = tall[0].shape[1]
    step = pl.program_id(0)
    count = n_ref[0]
    first_row = (2 * step + p_ref[0]) * TILE

    @pl.when(step == 0)
    def _():
        kp_ref[...] = jnp.zeros_like(kp_ref)
        loss_ref[...] = jnp.zeros_like(loss_ref)

    @pl.when(first_row >= count)
    def _():
        qp_ref[...] = jnp.zeros_like(qp_ref)

    @pl.when(first_row < count)
    def _():
        at = 0
        for kind in range(kinds):
            scale_t = LOG2E * tdims[kind] ** (-0.5)
            scale_s = LOG2E * sdims[kind] ** (-0.5)
            for own, every, d_ref, m_ref in (
                (town[kind], tall[kind], dt_ref, mt_ref),
                (sown[kind], sall[kind], ds_ref, ms_ref),
            ):
                left = own[...]
                top = jnp.full((TILE, LANES), -jnp.inf, jnp.float32)
                for c in range(0, seq, TILE):
                    d = lax.dot_general(
                        left,
                        every[:, c : c + TILE],
                        (((0,), (0,)), ((), ())),
                        preferred_element_type=jnp.float32,
                    )
                    d_ref[:, c : c + TILE] = d
                    for k in range(0, TILE, LANES):
                        top = jnp.maximum(top, d[:, k : k + LANES])
                m_ref[...] = jnp.broadcast_to(
                    jnp.max(top, axis=1, keepdims=True), (TILE, LANES)
                )

            def group(g, loss):
                rows = pl.ds(pl.multiple_of(g * GROUP, GROUP), GROUP)
                mt, ms = mt_ref[rows, :], ms_ref[rows, :]
                zt = jnp.zeros((GROUP, LANES), jnp.float32)
                zs = jnp.zeros((GROUP, LANES), jnp.float32)
                kl = jnp.zeros((GROUP, LANES), jnp.float32)
                for c in range(0, seq, LANES):
                    xt = (dt_ref[rows, c : c + LANES] - mt) * scale_t
                    xs = (ds_ref[rows, c : c + LANES] - ms) * scale_s
                    et, es = jnp.exp2(xt), jnp.exp2(xs)
                    zt, zs, kl = zt + et, zs + es, kl + et * (xt - xs)
                    dt_ref[rows, c : c + LANES] = et
                    ds_ref[rows, c : c + LANES] = es
                zt = jnp.sum(zt, axis=1, keepdims=True)
                zs = jnp.sum(zs, axis=1, keepdims=True)
                kl = jnp.sum(kl, axis=1, keepdims=True)
                row = first_row + g * GROUP + lax.broadcasted_iota(jnp.int32, (GROUP, 1), 0)
                valid = row < count
                loss = loss + jnp.where(valid, kl / zt * LN2 + jnp.log(zs) - jnp.log(zt), 0.0)
                rt = jnp.broadcast_to(jnp.where(valid, 1.0 / zt, 0.0), (GROUP, LANES))
                rs = jnp.broadcast_to(jnp.where(valid, 1.0 / zs, 0.0), (GROUP, LANES))
                for c in range(0, seq, LANES):
                    w_ref[rows, c : c + LANES] = (
                        ds_ref[rows, c : c + LANES] * rs - dt_ref[rows, c : c + LANES] * rt
                    ).astype(jnp.bfloat16)
                return loss

            loss = lax.fori_loop(
                0, TILE // GROUP, group, jnp.zeros((GROUP, 1), jnp.float32)
            )
            loss_ref[...] += jnp.broadcast_to(loss, loss_ref.shape)
            width = sdims[kind]
            qp_ref[at : at + width, :] = lax.dot_general(
                sall[kind][...],
                w_ref[...],
                (((1,), (1,)), ((), ())),
                preferred_element_type=jnp.float32,
            )[:width]
            left = sown[kind][...]
            for c in range(0, seq, 2 * TILE):
                kp_ref[at : at + width, c : c + 2 * TILE] += lax.dot_general(
                    left,
                    w_ref[:, c : c + 2 * TILE],
                    (((1,), (0,)), ((), ())),
                    preferred_element_type=jnp.float32,
                )[:width]
            at += width


def relations(count, half, tdims, sdims, town, sown, tall, sall):
    seq = tall[0].shape[1]
    mine = town[0].shape[1]
    total = sum(sdims)
    block = lambda a: pl.BlockSpec((a.shape[0], TILE), lambda i: (0, i))
    whole = lambda a: pl.BlockSpec(a.shape, lambda i: (0, 0))
    smem = pl.BlockSpec(memory_space=pltpu.SMEM)
    return pl.pallas_call(
        functools.partial(relation_kernel, tdims, sdims),
        grid=(mine // TILE,),
        in_specs=[smem, smem]
        + [block(a) for a in town + sown]
        + [whole(a) for a in tall + sall],
        out_specs=[
            pl.BlockSpec((total, TILE), lambda i: (0, i)),
            pl.BlockSpec((total, seq), lambda i: (0, 0)),
            pl.BlockSpec((GROUP, LANES), lambda i: (0, 0)),
        ],
        out_shape=[
            jax.ShapeDtypeStruct((total, mine), jnp.float32),
            jax.ShapeDtypeStruct((total, seq), jnp.float32),
            jax.ShapeDtypeStruct((GROUP, LANES), jnp.float32),
        ],
        scratch_shapes=[
            pltpu.VMEM((TILE, seq), jnp.float32),
            pltpu.VMEM((TILE, seq), jnp.float32),
            pltpu.VMEM((TILE, LANES), jnp.float32),
            pltpu.VMEM((TILE, LANES), jnp.float32),
            pltpu.VMEM((TILE, seq), jnp.bfloat16),
        ],
        compiler_params=pltpu.CompilerParams(vmem_limit_bytes=40 * 2**20),
        cost_estimate=pl.CostEstimate(
            flops=len(tdims) * 10_000_000_000, bytes_accessed=4 * 2**20, transcendentals=0
        ),
    )(count, half, *town, *sown, *tall, *sall)


def gather_kernel(x_ref, o_ref, here, send, recv):
    zl, y, c = (lax.axis_index(a) for a in HEAD)
    ny = lax.axis_size(HEAD[1])
    size = x_ref.shape[0]
    low, high = pl.ds(0, size // 2), pl.ds(size // 2, size // 2)
    up, down, far = lax.rem(y + 1, ny), lax.rem(y + ny - 1, ny), lax.rem(y + 2, ny)
    sibling, across = {HEAD[2]: 1 - c}, {HEAD[0]: 1 - zl}
    above, below = {HEAD[1]: up}, {HEAD[1]: down}
    slot = lambda z, at: (z * ny + at) * 2 + c
    barrier = pltpu.get_barrier_semaphore()
    for device in (sibling, across, above, below):
        pl.semaphore_signal(
            barrier, inc=1, device_id=device, device_id_type=pl.DeviceIdType.MESH
        )
    pl.semaphore_wait(barrier, 4)
    copies = []

    def push(source, target, device):
        k = len(copies)
        copy = pltpu.make_async_remote_copy(
            src_ref=source,
            dst_ref=target,
            send_sem=send.at[k],
            recv_sem=recv.at[k],
            device_id=device,
            device_id_type=pl.DeviceIdType.MESH,
        )
        copy.start()
        copies.append(copy)
        return copy

    def forward(index, device, part=None):
        place = o_ref.at[index] if part is None else o_ref.at[index, part]
        return push(place, place, device)

    own = o_ref.at[slot(zl, y)]
    first = push(x_ref, own, across)
    from_down = push(x_ref, own, above)
    from_up = push(x_ref, own, below)
    last = [push(x_ref, own, sibling)]
    keep = pltpu.make_async_copy(x_ref, own, here)
    keep.start()
    first.wait_recv()
    z = 1 - zl
    cross_down = forward(slot(z, y), above)
    cross_up = forward(slot(z, y), below)
    last.append(forward(slot(z, y), sibling))
    halves = []
    for plane, lower, upper in ((zl, from_down, from_up), (z, cross_down, cross_up)):
        lower.wait_recv()
        half_a = forward(slot(plane, down), above, low)
        last.append(forward(slot(plane, down), sibling))
        upper.wait_recv()
        half_b = forward(slot(plane, up), below, high)
        last.append(forward(slot(plane, up), sibling))
        halves.append((plane, half_a, half_b))
    for plane, half_a, half_b in halves:
        half_a.wait_recv()
        half_b.wait_recv()
        last.append(forward(slot(plane, far), sibling))
    for copy in last:
        copy.wait_recv()
    for copy in copies:
        copy.wait_send()
    keep.wait()


def gathered(x, collective_id):
    count = lax.axis_size(HEAD)
    return pl.pallas_call(
        gather_kernel,
        out_shape=jax.ShapeDtypeStruct((count, *x.shape), x.dtype),
        in_specs=[pl.BlockSpec(memory_space=pltpu.VMEM)],
        out_specs=pl.BlockSpec(memory_space=pltpu.VMEM),
        scratch_shapes=[
            pltpu.SemaphoreType.DMA,
            pltpu.SemaphoreType.DMA((17,)),
            pltpu.SemaphoreType.DMA((17,)),
        ],
        compiler_params=pltpu.CompilerParams(
            collective_id=collective_id, has_side_effects=True, vmem_limit_bytes=24 * 2**20
        ),
        cost_estimate=pl.CostEstimate(
            flops=10_000_000_000, bytes_accessed=count * x.size * 2, transcendentals=0
        ),
    )(x)


def own_tokens(rows, half):
    cut = rows.reshape(rows.shape[0], -1, 2, TILE)
    return lax.dynamic_index_in_dim(cut, half, 2, keepdims=False).reshape(rows.shape[0], -1)


def columns_of_heads(parts, heads, pad):
    feats = parts[0].shape[0]
    joined = jnp.concatenate([a.reshape(feats, heads, -1) for a in parts], axis=2)
    joined = jnp.pad(joined, ((0, 0), (0, 0), (0, pad - joined.shape[2])))
    return joined.reshape(feats, -1)


def with_mask_row(rows, last):
    count = rows.shape[0]
    pad = -(count + 1) % 16
    return jnp.concatenate(
        [rows, last[None].astype(rows.dtype), jnp.zeros((pad, rows.shape[1]), rows.dtype)]
    )


def pieces(value):
    out = []
    for _ in range(3):
        top = lax.reduce_precision(value, 8, 7)
        out.append(top.astype(jnp.bfloat16))
        value = value - top
    return jnp.stack(out)


def copy_for_each(value, axis):
    size = lax.axis_size(axis)
    return lax.all_to_all(
        jnp.broadcast_to(value[None], (size, *value.shape)), axis, 0, 0, tiled=True
    )


def per_device(
    token_ids, teacher_hidden, teacher_query, teacher_kv, student_hidden, student_query, student_kv
):
    seq_len = token_ids.shape[0]
    heads = lax.axis_size(HEAD)
    local_heads = HEADS // heads
    rows = lax.axis_size(ROW)
    half = lax.axis_index(ROW) % 2
    swap = [(i, i ^ 1) for i in range(lax.axis_size(ROW[1]))]
    valid_mask = token_ids != pad_token
    count = jnp.sum(valid_mask.astype(jnp.int32))
    bias = jnp.where(valid_mask, 0.0, neg_fill)
    ones = jnp.ones((seq_len // 2,), jnp.float32)

    tq, tk = teacher_query.shape[1] // local_heads, teacher_kv.shape[2] // local_heads
    sq, sk = student_query.shape[1] // local_heads, student_kv.shape[2] // local_heads
    q_pad = sq + -sq % 16
    s_pad = q_pad + 2 * sk
    student_parts = [student_query, student_kv[:, 0], student_kv[:, 1]]
    student_weight = columns_of_heads(student_parts, local_heads, s_pad)
    teacher_kv_weight = columns_of_heads([teacher_kv[:, 0], teacher_kv[:, 1]], local_heads, 2 * tk)

    def project(weight, feats):
        return lax.dot_general(
            weight, feats, (((0,), (1,)), ((), ())), preferred_element_type=jnp.float32
        )

    def swapped(own):
        other = lax.ppermute(own, ROW[1], swap)
        low = jnp.where(half == 0, own, other)
        high = jnp.where(half == 0, other, own)
        return jnp.concatenate([low, high])

    def summed(arrived):
        return swapped(arrived.sum(axis=0).astype(jnp.bfloat16))

    for_rows = lambda part: part.reshape(rows, -1, seq_len)
    both = jnp.concatenate([teacher_hidden, student_hidden], axis=1)
    feats = gathered(both, 0).reshape(seq_len, -1)
    teacher_feats = feats[:, : teacher_hidden.shape[1]]
    student_feats = feats[:, teacher_hidden.shape[1] :]
    first = jnp.concatenate(
        [
            for_rows(project(student_weight, student_feats)),
            for_rows(project(teacher_kv_weight, teacher_feats)),
        ],
        axis=1,
    )
    first_rows = summed(lax.all_to_all(first, ROW, split_axis=0, concat_axis=0, tiled=True))
    cut = first_rows.reshape(2, -1, seq_len)
    student_rows = cut[:, : local_heads * s_pad // rows].reshape(-1, seq_len)
    teacher_kv_rows = cut[:, local_heads * s_pad // rows :].reshape(-1, seq_len)
    second = for_rows(project(teacher_query, teacher_feats))
    spread = jnp.concatenate(
        [
            columns_of_heads(student_parts[:1], local_heads, q_pad).T,
            columns_of_heads(student_parts[1:], local_heads, 2 * sk).T,
        ]
    )
    second, student_rows, teacher_kv_rows, spread = lax.optimization_barrier(
        (second, student_rows, teacher_kv_rows, spread)
    )
    all_weight = gathered(spread, 1)
    arrived = lax.all_to_all(second, ROW, split_axis=0, concat_axis=0, tiled=True)
    arrived, all_weight = lax.optimization_barrier((arrived, all_weight))
    teacher_q_rows = summed(arrived)

    def relate(tparts, sparts):
        every = lambda parts: [with_mask_row(a, bias) for a in parts]
        mine = lambda parts: [with_mask_row(own_tokens(a, half), ones) for a in parts]
        tdims, sdims = tuple(a.shape[0] for a in tparts), tuple(a.shape[0] for a in sparts)
        query_part, key_part, loss = relations(
            count[None],
            half[None].astype(jnp.int32),
            tdims,
            sdims,
            mine(tparts),
            mine(sparts),
            every(tparts),
            every(sparts),
        )
        from_other = lax.ppermute(own_tokens(key_part, 1 - half), ROW[1], swap)
        scale = jnp.concatenate([jnp.full((d, 1), d ** (-0.5), jnp.float32) for d in sdims])
        grad = (query_part + own_tokens(key_part, half) + from_other) * scale
        return grad.astype(jnp.bfloat16), jnp.sum(loss[:, 0])

    def shared(grad):
        arrived = copy_for_each(grad, ROW)
        cut = arrived.reshape(local_heads, 2, grad.shape[0], -1, TILE // LANES, LANES)
        return cut.transpose(3, 1, 4, 0, 2, 5).reshape(heads, -1, LANES)

    def weight_grads(blocks):
        by_column = jnp.moveaxis(blocks, 0, 1).reshape(blocks.shape[1], seq_len)
        return lax.dot_general(
            student_feats, by_column, (((0,), (1,)), ((), ())), preferred_element_type=jnp.float32
        ).reshape(student_feats.shape[1], local_heads, -1)

    def token_grads(blocks, weight):
        got = lax.all_to_all(blocks, HEAD, split_axis=0, concat_axis=0, tiled=True)
        flat = got.reshape(-1, got.shape[2])
        return got, lax.dot_general(
            flat,
            weight.reshape(flat.shape[0], -1),
            (((0,), (0,)), ((), ())),
            preferred_element_type=jnp.float32,
        )

    kv_grad, kv_loss = relate(
        [teacher_kv_rows[:tk], teacher_kv_rows[tk:]],
        [student_rows[sq : sq + sk], student_rows[sq + sk : sq + 2 * sk]],
    )
    kv_blocks = shared(kv_grad)
    kv_out = (
        weight_grads(kv_blocks)
        .reshape(-1, local_heads, 2, sk)
        .transpose(0, 2, 1, 3)
        .reshape(student_kv.shape)
    )
    _, kv_input = token_grads(kv_blocks, all_weight[:, local_heads * q_pad :])

    q_grad, q_loss = relate([teacher_q_rows], [student_rows[:sq]])
    loss = q_loss + kv_loss
    loss = pieces(loss + lax.ppermute(loss, ROW[1], swap))
    last = jnp.zeros((q_pad - sq, q_grad.shape[1] // LANES, LANES), jnp.bfloat16)
    last = last.at[0, :, :3].set(jnp.broadcast_to(loss, (last.shape[1], 3)))
    q_blocks = shared(jnp.concatenate([q_grad, last.reshape(q_pad - sq, -1)]))
    query_out = weight_grads(q_blocks)[:, :, :sq].reshape(student_query.shape)
    got, q_input = token_grads(q_blocks, all_weight[:, : local_heads * q_pad])
    kl_sum = jnp.sum(got.reshape(heads, local_heads, q_pad, LANES)[:, :, sq, :3].astype(jnp.float32))
    mean_kl = kl_sum / (3.0 * HEADS * count.astype(jnp.float32))
    return (mean_kl, query_out, kv_out, kv_input + q_input)


def solution(mesh):
    finer = Mesh(
        mesh.devices.reshape(2, 4, 2, 2, 4), ("head_0", "head_1", "head_2", "row_0", "row_1")
    )
    in_specs = (
        P(),
        P(HEAD, ROW),
        P(ROW, HEAD),
        P(ROW, None, HEAD),
        P(HEAD, ROW),
        P(ROW, HEAD),
        P(ROW, None, HEAD),
    )
    out_specs = (P(), P(ROW, HEAD), P(ROW, None, HEAD), P(HEAD, ROW))
    return jax.shard_map(
        per_device, mesh=finer, in_specs=in_specs, out_specs=out_specs, check_vma=False
    )
```
